32 devices in a mesh: dp: 8 (over y, x, core), tensor: 4 (over z).
Axes of the slice: x: 2, y: 2, z: 4, core: 2. Of those that a mesh axis runs over, the one named last changes fastest.
Arguments:
- teacher_in: bfloat16 [2048, 2048], P('dp'), may hold values from -13 to 13
- teacher_gain: float32 [2, 2048], replicated, may hold values from 0.25 to 1.75
- t_gate: bfloat16 [2, 2048, 5472], P(None, 'dp', 'tensor'), may hold values from -0.125 to 0.125
- t_up: bfloat16 [2, 2048, 5472], P(None, 'dp', 'tensor'), may hold values from -0.125 to 0.125
- t_down: bfloat16 [2, 5472, 2048], P(None, 'tensor', 'dp'), may hold values from -0.078125 to 0.078125
- student_in: bfloat16 [2048, 1024], P('dp'), may hold values from -13 to 13
- student_gain: float32 [2, 1024], replicated, may hold values from 0.3 to 3.5
- s_gate: bfloat16 [2, 1024, 4096], P(None, None, 'tensor'), may hold values from -0.1875 to 0.1875
- s_up: bfloat16 [2, 1024, 4096], P(None, None, 'tensor'), may hold values from -0.1875 to 0.1875
- s_down: bfloat16 [2, 4096, 1024], P(None, 'tensor'), may hold values from -0.09375 to 0.09375
- proj: bfloat16 [1024, 2048], P(None, 'tensor'), may hold values from -1 to 1
- layer_map: int32 [2], replicated, may hold values from 0 to 1, each once
Outputs:
- teacher_states: bfloat16 [2, 2048, 2048], P(None, ('dp', 'tensor'))
- grad_gate: float32 [2, 1024, 4096], P(None, 'dp', 'tensor')
- grad_up: float32 [2, 1024, 4096], P(None, 'dp', 'tensor')
- grad_down: float32 [2, 4096, 1024], P(None, 'tensor', 'dp')
- grad_proj: float32 [1024, 2048], P('dp', 'tensor')
- mean_error: float32 [2], replicated
- grad_rms: float32 [4], replicated
The draws below stay inside these ranges and needn't reach their ends.
Inputs may be any that keep to these rules, and one draw needn't show every extreme that they name: `layer_map`: each teacher sublayer is matched to exactly one student sublayer.
All inputs are finite; a program needn't handle non-finite values.
Results may differ from the reference program's by a relative error of at most 0.02.
Values may be sent and summed in bfloat16 or wider, within the bound.
No kernel may reach another device: no remote copies, remote signals or barrier semaphores. Data moves between devices by JAX's collectives and lax.ppermute only.
A program may use at most 128 MiB of HBM per device.

```python
import math
import jax
import jax.numpy as jnp
from jax import lax

DT = 2048
FT = 5472
DS = 1024
FS = 4096
T_LAYERS = 2
S_LAYERS = 2
SEQ = 512
TOK_DEV = 256
TOKENS = 2048
N_DP = 8
N_TENSOR = 4


def rising(count, low, high):
    ramp = jnp.linspace(0.0, 1.0, count, dtype=jnp.float32)
    return jnp.exp(math.log(low) + ramp * (math.log(high) - math.log(low)))


def base_noise(key, shape):
    return jnp.clip(jax.random.normal(key, shape, jnp.float32), -4.0, 4.0)


def draw_teacher_in(key, part):
    first, second = jax.random.split(jax.random.fold_in(key, 11))
    ramp = rising(TOKENS, 0.5, 2.5)
    rows = ramp[:, None] * jax.random.uniform(second, (TOKENS, 1), jnp.float32, 0.8, 1.2)
    return (base_noise(first, (TOKENS, DT)) * rows).astype(jnp.bfloat16)


def draw_student_in(key, part):
    first, second = jax.random.split(jax.random.fold_in(key, 23))
    ramp = rising(DS, 0.5, 2.5)
    columns = ramp[None, :] * jax.random.uniform(second, (1, DS), jnp.float32, 0.8, 1.2)
    return (base_noise(first, (TOKENS, DS)) * columns).astype(jnp.bfloat16)


def draw_student_gain(key, part):
    inner = jax.random.fold_in(key, 37)
    ramp = rising(DS, 0.5, 2.0)
    jitter = jax.random.uniform(inner, (S_LAYERS, DS), jnp.float32, 0.85, 1.15)
    return (ramp[None, :] * jitter).astype(jnp.float32)


def draw_proj(key, part):
    first, second = jax.random.split(jax.random.fold_in(key, 41))
    ramp = rising(DS, 0.5, 2.0)
    rows = ramp[:, None] * jax.random.uniform(second, (DS, 1), jnp.float32, 0.85, 1.15) / math.sqrt(DS)
    return (base_noise(first, (DS, DT)) * rows).astype(jnp.bfloat16)


def level_of(stream_key, shape, pieces, least, largest):
    def one(position, parts):
        steps = jax.random.uniform(jax.random.fold_in(jax.random.fold_in(stream_key, 6), position), (parts,), jnp.float32, least / len(pieces), largest / len(pieces))
        return jnp.repeat(jnp.exp(steps), shape[position] // parts).reshape((-1,) + (1,) * (len(shape) - position - 1))

    level = one(*pieces[0])
    for cut in pieces[1:]:
        level = level * one(*cut)
    return level


def normal_values(rng, shape, deviation, most, cuts=(), kind=jnp.bfloat16):
    drawn = jax.random.normal(rng, shape, jnp.float32) * deviation
    if len(cuts) > 0:
        drawn = level_of(rng, shape, cuts, -0.22, 0.18) * drawn
    return jnp.clip(drawn, min=-most, max=most).astype(kind)


def setup_inputs(seed: int = 0) -> dict:
    splits = jax.random.split(jax.random.key(seed), 13)
    return {
        "teacher_in": draw_teacher_in(jax.random.fold_in(splits[12], 71), 0),
        "teacher_gain": jnp.clip(1.0 + 0.15 * jax.random.normal(splits[1], (T_LAYERS, DT), jnp.float32), 0.25, 1.75),
        "t_gate": normal_values(splits[2], (T_LAYERS, DT, FT), DT ** -0.5, 0.125, ((1, 8), (2, 4))),
        "t_up": normal_values(splits[3], (T_LAYERS, DT, FT), DT ** -0.5, 0.125, ((1, 8), (2, 4))),
        "t_down": normal_values(splits[4], (T_LAYERS, FT, DT), FT ** -0.5, 0.078125, ((1, 4), (2, 8))),
        "student_in": draw_student_in(jax.random.fold_in(splits[12], 71), 0),
        "student_gain": draw_student_gain(jax.random.fold_in(splits[12], 71), 0),
        "s_gate": normal_values(splits[7], (S_LAYERS, DS, FS), DS ** -0.5, 0.1875, ((2, 4),)),
        "s_up": normal_values(splits[8], (S_LAYERS, DS, FS), DS ** -0.5, 0.1875, ((2, 4),)),
        "s_down": normal_values(splits[9], (S_LAYERS, FS, DS), FS ** -0.5, 0.09375, ((1, 4),)),
        "proj": draw_proj(jax.random.fold_in(splits[12], 71), 0),
        "layer_map": jax.random.permutation(splits[11], T_LAYERS).astype(jnp.int32),
    }


EPSILON = 1e-05

def inverse_rms(values):
    return lax.rsqrt(lax.optimization_barrier(jnp.mean(values * values, axis=-1, keepdims=True)) + EPSILON)

def contract_rows(left, right):
    return lax.dot_general(left, right, (((0,), (0,)), ((), ())), preferred_element_type=jnp.float32)

def contract_cols(left, right):
    return lax.dot_general(left, right, (((1,), (1,)), ((), ())), preferred_element_type=jnp.float32)

def rounded(values):
    narrow = lax.optimization_barrier(values.astype(jnp.bfloat16))
    return narrow.astype(jnp.float32)

def reference(teacher_in, teacher_gain, t_gate, t_up, t_down, student_in, student_gain, s_gate, s_up, s_down, proj, layer_map):
    block_width = FT // N_TENSOR
    state = teacher_in
    outputs = []
    for k in range(T_LAYERS):
        state_wide = state.astype(jnp.float32)
        normed = (state_wide * inverse_rms(state_wide) * teacher_gain[k]).astype(jnp.bfloat16)
        gate_act = jnp.dot(normed, t_gate[k], preferred_element_type=jnp.float32)
        up_act = jnp.dot(normed, t_up[k], preferred_element_type=jnp.float32)
        hidden = (jax.nn.silu(gate_act) * up_act).astype(jnp.bfloat16)
        summed = jnp.zeros_like(state_wide)
        for j in range(N_TENSOR):
            term = jnp.dot(hidden[:, j * block_width:(j + 1) * block_width], t_down[k, j * block_width:(j + 1) * block_width], preferred_element_type=jnp.float32)
            summed = summed + rounded(term)
        state = (state_wide + summed).astype(jnp.bfloat16)
        outputs.append(state)
    teacher_states = jnp.stack(outputs)
    states = [student_in]
    normeds, gates, ups, units, scales = ([], [], [], [], [])
    for l in range(S_LAYERS):
        wide = states[l].astype(jnp.float32)
        scale = inverse_rms(wide)
        normed = (wide * scale * student_gain[l]).astype(jnp.bfloat16)
        gate_act = jnp.dot(normed, s_gate[l], preferred_element_type=jnp.float32)
        up_act = jnp.dot(normed, s_up[l], preferred_element_type=jnp.float32)
        units_now = (jax.nn.silu(gate_act) * up_act).astype(jnp.bfloat16)
        result = wide + jnp.dot(units_now, s_down[l], preferred_element_type=jnp.float32)
        states.append(result.astype(jnp.bfloat16))
        normeds.append(normed)
        gates.append(gate_act)
        ups.append(up_act)
        units.append(units_now)
        scales.append(scale)
    error_sums = []
    deltas = []
    for l in range(S_LAYERS):
        predicted = jnp.dot(states[l + 1], proj, preferred_element_type=jnp.float32)
        target = lax.dynamic_index_in_dim(teacher_states, layer_map[l], 0, keepdims=False).astype(jnp.float32)
        errors = predicted - target
        error_sums.append(jnp.sum(errors * errors))
        deltas.append((errors * (2.0 / (S_LAYERS * SEQ))).astype(jnp.bfloat16))
    grad_x = contract_cols(deltas[S_LAYERS - 1], proj)
    out_grads = [None] * S_LAYERS
    gate_grads = [None] * S_LAYERS
    up_grads = [None] * S_LAYERS
    for l in reversed(range(S_LAYERS)):
        grad_out = grad_x.astype(jnp.bfloat16)
        grad_units = contract_cols(grad_out, s_down[l])
        sigma = jax.nn.sigmoid(gates[l])
        grad_gate_act = (grad_units * ups[l] * sigma * (1.0 + gates[l] * (1.0 - sigma))).astype(jnp.bfloat16)
        grad_up_act = (grad_units * jax.nn.silu(gates[l])).astype(jnp.bfloat16)
        out_grads[l] = grad_out
        gate_grads[l] = grad_gate_act
        up_grads[l] = grad_up_act
        if l > 0:
            grad_norm = contract_cols(grad_gate_act, s_gate[l]) + contract_cols(grad_up_act, s_up[l])
            wide = states[l].astype(jnp.float32)
            scaled = grad_norm * student_gain[l]
            through = scales[l] * scaled - wide * scales[l] ** 3 * lax.optimization_barrier(jnp.mean(wide * scaled, axis=-1, keepdims=True))
            grad_x = grad_x + through + contract_cols(deltas[l - 1], proj)
    grad_gate = jnp.zeros((S_LAYERS, DS, FS), jnp.float32)
    grad_up = jnp.zeros((S_LAYERS, DS, FS), jnp.float32)
    grad_down = jnp.zeros((S_LAYERS, FS, DS), jnp.float32)
    grad_proj = jnp.zeros((DS, DT), jnp.float32)
    for g in range(N_DP):
        low = g * TOK_DEV
        high = low + TOK_DEV
        proj_part = jnp.zeros((DS, DT), jnp.float32)
        for l in range(S_LAYERS):
            grad_gate = grad_gate.at[l].add(rounded(contract_rows(normeds[l][low:high], gate_grads[l][low:high])))
            grad_up = grad_up.at[l].add(rounded(contract_rows(normeds[l][low:high], up_grads[l][low:high])))
            grad_down = grad_down.at[l].add(rounded(contract_rows(units[l][low:high], out_grads[l][low:high])))
            proj_part = proj_part + contract_rows(states[l + 1][low:high], deltas[l][low:high])
        grad_proj = grad_proj + rounded(proj_part)
    squares = jnp.stack([jnp.sum(grad_gate * grad_gate), jnp.sum(grad_up * grad_up), jnp.sum(grad_down * grad_down), jnp.sum(grad_proj * grad_proj)])
    counts = jnp.array([S_LAYERS * DS * FS, S_LAYERS * DS * FS, S_LAYERS * DS * FS, DS * DT], jnp.float32)
    mean_error = jnp.stack(error_sums) / (TOKENS * DT)
    grad_rms = jnp.sqrt(squares / counts)
    return (teacher_states, grad_gate, grad_up, grad_down, grad_proj, mean_error, grad_rms)
```

```python
import jax
import jax.numpy as jnp
from jax import lax
from jax.sharding import Mesh
from jax.sharding import PartitionSpec as P

SEQ = 512
EPSILON = 1e-05
F32 = jnp.float32
BF16 = jnp.bfloat16
CHIP = ("row", "col")


def inverse_rms(values):
    return lax.rsqrt(jnp.mean(values * values, axis=-1, keepdims=True) + EPSILON)


def dot(left, right):
    return jnp.dot(left, right, preferred_element_type=F32)


def contract_rows(left, right):
    return lax.dot_general(left, right, (((0,), (0,)), ((), ())), preferred_element_type=F32)


def contract_cols(left, right):
    return lax.dot_general(left, right, (((1,), (1,)), ((), ())), preferred_element_type=F32)


def pull(value, axis, shift):
    n = lax.axis_size(axis)
    return lax.ppermute(value, axis, [(j, (j - shift) % n) for j in range(n)])


def push(value, axis, shift):
    n = lax.axis_size(axis)
    return lax.ppermute(value, axis, [(j, (j + shift) % n) for j in range(n)])


def swap(value):
    return lax.ppermute(value, "core", [(0, 1), (1, 0)])


def chip_shifts():
    return [(r, c) for r in range(lax.axis_size("row")) for c in range(lax.axis_size("col"))]


def push_chip(value, shift):
    rows, cols = lax.axis_size("row"), lax.axis_size("col")
    pairs = [
        (r * cols + c, ((r + shift[0]) % rows) * cols + (c + shift[1]) % cols)
        for r in range(rows)
        for c in range(cols)
    ]
    return lax.ppermute(value, CHIP, pairs)


def chip_index(shift):
    rows, cols = lax.axis_size("row"), lax.axis_size("col")
    row = lax.rem(lax.axis_index("row") + shift[0], rows)
    col = lax.rem(lax.axis_index("col") + shift[1], cols)
    return row * cols + col


def gather_chips(block, axis):
    half = block.shape[axis] // 2
    rows, cols = lax.axis_size("row"), lax.axis_size("col")
    found = {(0, 0): block}
    for c in range(1, cols):
        found[(0, c)] = pull(block, "col", c)
    for r in range(1, rows):
        found[(r, 0)] = pull(block, "row", r)
    for r in range(1, rows):
        for c in range(1, cols):
            first = lax.slice_in_dim(found[(0, c)], 0, half, axis=axis)
            last = lax.slice_in_dim(found[(r, 0)], half, None, axis=axis)
            found[(r, c)] = jnp.concatenate(
                [pull(first, "row", r), pull(last, "col", c)], axis=axis
            )
    return [found[s] for s in chip_shifts()]


def take_blocks(value, axis, width, starts):
    return jnp.concatenate(
        [lax.dynamic_slice_in_dim(value, s * width, width, axis) for s in starts], axis=axis
    )


def per_device(
    teacher_in,
    teacher_gain,
    t_gate,
    t_up,
    t_down,
    student_in,
    student_gain,
    s_gate,
    s_up,
    s_down,
    proj,
    layer_map,
):
    n = lax.axis_size("tensor")
    pos = lax.axis_index("tensor")
    core = lax.axis_index("core")
    shifts = chip_shifts()
    chips = len(shifts)
    t_layers = t_gate.shape[0]
    s_layers = s_gate.shape[0]
    tokens, dt = teacher_in.shape
    ds = student_in.shape[1]
    own = tokens // n
    share = dt // (2 * chips)
    positions = [lax.rem(pos + k, n) for k in range(n)]
    groups = [chip_index(s) for s in shifts]
    mine_cols = [g * 2 + core for g in groups]
    other_cols = [g * 2 + 1 - core for g in groups]

    def sum_rows(part):
        total = part[:own].astype(F32)
        for k in range(1, n):
            total = total + push(part[k * own : (k + 1) * own], "tensor", k).astype(F32)
        return total

    def gather_rows(rows):
        return jnp.concatenate([rows] + [pull(rows, "tensor", k) for k in range(1, n)])

    weights = []
    for k in range(t_layers):
        weights.append(
            (
                gather_chips(t_gate[k], 0),
                gather_chips(t_up[k], 0),
                gather_chips(t_down[k], 1),
            )
        )

    x = take_blocks(student_in, 0, own, positions)
    states, x_rows = [x], [x[:own].astype(F32)]
    normeds, gates, ups, units, scales = [], [], [], [], []
    for l in range(s_layers):
        wide = states[l].astype(F32)
        scale = inverse_rms(wide)
        normed = (wide * scale * student_gain[l]).astype(BF16)
        gate_act = dot(normed, s_gate[l])
        up_act = dot(normed, s_up[l])
        unit = (jax.nn.silu(gate_act) * up_act).astype(BF16)
        part = dot(unit, s_down[l]).astype(BF16)
        next_rows = (x_rows[l] + sum_rows(part)).astype(BF16)
        x_rows.append(next_rows.astype(F32))
        states.append(gather_rows(next_rows))
        normeds.append(normed)
        gates.append(gate_act)
        ups.append(up_act)
        units.append(unit)
        scales.append(scale)

    proj_mine = lax.dynamic_slice_in_dim(proj, core * share, share, 1)
    proj_cols = jnp.concatenate(
        [proj_mine] + [pull(proj_mine, "tensor", k) for k in range(1, n)], axis=1
    )
    predicted = []
    for l in range(s_layers):
        rows = x_rows[l + 1].astype(BF16)
        predicted.append(dot(jnp.concatenate([rows, swap(rows)]), proj_cols))

    wide = teacher_in.astype(F32)
    normed = (wide * inverse_rms(wide) * teacher_gain[0]).astype(BF16)
    normed = take_blocks(normed, 0, own, positions)
    kept = take_blocks(normed, 1, share, mine_cols)
    given = take_blocks(normed, 1, share, other_cols)
    normed = jnp.concatenate([kept, swap(given)])
    rows = lax.dynamic_slice_in_dim(teacher_in, pos * own, own, 0)
    state = jnp.concatenate(
        [take_blocks(rows, 1, share, mine_cols), swap(take_blocks(rows, 1, share, other_cols))]
    ).astype(F32)
    gain_mine = take_blocks(teacher_gain, 1, share, mine_cols)
    home = [lax.axis_index("row"), lax.axis_index("col")]

    def to_plain(value, first):
        rows_n, cols_n = lax.axis_size("row"), lax.axis_size("col")
        picked = []
        for k in range(chips):
            chip = lax.rem(first + k, chips)
            r = lax.rem(chip // cols_n - home[0] + rows_n, rows_n)
            c = lax.rem(lax.rem(chip, cols_n) - home[1] + cols_n, cols_n)
            picked.append(r * cols_n + c)
        return take_blocks(value, 1, share, picked)

    out_states, targets = [], []
    for k in range(t_layers):
        w_gate, w_up, w_down = weights[k]
        acts = []
        for w in (w_gate, w_up):
            total = dot(normed[:, :share], w[0])
            for i in range(1, chips):
                total = total + dot(normed[:, i * share : (i + 1) * share], w[i])
            acts.append(total[:tokens] + swap(total[tokens:]))
        hidden = (jax.nn.silu(acts[0]) * acts[1]).astype(BF16)
        both = jnp.concatenate([hidden, swap(hidden)])
        part = jnp.concatenate([dot(both, w).astype(BF16) for w in w_down], axis=1)

        def rows_of(j):
            return jnp.concatenate(
                [part[j * own : (j + 1) * own], part[tokens + j * own : tokens + (j + 1) * own]]
            )

        total = rows_of(0).astype(F32)
        for j in range(1, n):
            total = total + push(rows_of(j), "tensor", j).astype(F32)
        narrow = (state + total).astype(BF16)
        state = narrow.astype(F32)
        if k + 1 < t_layers:
            squares = jnp.sum(state * state, axis=-1, keepdims=True)
            across = swap(jnp.concatenate([squares[own:], squares[:own]]))
            inv = lax.rsqrt((squares + across) / dt + EPSILON)
            block = (state * inv * gain_mine[k + 1]).astype(BF16)
            blocks = [block] + [pull(block, "tensor", j) for j in range(1, n)]
            normed = jnp.concatenate([b[:own] for b in blocks] + [b[own:] for b in blocks])
        targets.append(to_plain(narrow, pos))
        mine = to_plain(narrow[:own], 0)
        theirs = swap(to_plain(narrow[own:], 0))
        lower = jnp.where(core == 0, mine, theirs)
        upper = jnp.where(core == 0, theirs, mine)
        pieces = []
        for j in range(chips):
            pieces.append(lower[:, j * share : (j + 1) * share])
            pieces.append(upper[:, j * share : (j + 1) * share])
        out_states.append(jnp.concatenate(pieces, axis=1))
    targets = jnp.stack(targets)

    error_parts, deltas, c_rows = [], [], []
    for l in range(s_layers):
        target = lax.dynamic_index_in_dim(targets, layer_map[l], 0, keepdims=False)
        errors = predicted[l] - target.astype(F32)
        error_parts.append(jnp.sum(errors * errors))
        deltas.append((errors * (2.0 / (s_layers * SEQ))).astype(BF16))
    for l in range(s_layers):
        part = contract_cols(deltas[l], proj_cols)
        c_rows.append(part[:own] + swap(part[own:]))

    ds_mine = [g * 2 + core for g in groups]
    ds_other = [g * 2 + 1 - core for g in groups]
    slot = ds // (2 * chips)

    def by_owner(value):
        return take_blocks(value, 1, slot, ds_mine + ds_other)

    def reduce_blocks(blocks):
        total = blocks[0]
        for s, b in zip(shifts[1:], blocks[1:]):
            total = total + push_chip(b.astype(BF16), s).astype(F32)
        return total

    gate_grads = [None] * s_layers
    up_grads = [None] * s_layers
    down_grads = [None] * s_layers
    grad_rows = c_rows[s_layers - 1]
    for l in reversed(range(s_layers)):
        grad_out = gather_rows(grad_rows.astype(BF16))
        grad_units = contract_cols(grad_out, s_down[l])
        sigma = jax.nn.sigmoid(gates[l])
        grad_gate_act = (
            grad_units * ups[l] * sigma * (1.0 + gates[l] * (1.0 - sigma))
        ).astype(BF16)
        grad_up_act = (grad_units * jax.nn.silu(gates[l])).astype(BF16)
        if l > 0:
            norm_part = contract_cols(grad_gate_act, s_gate[l]) + contract_cols(
                grad_up_act, s_up[l]
            )
            grad_norm = sum_rows(norm_part.astype(BF16))
            wide = x_rows[l]
            scale = scales[l][:own]
            scaled = grad_norm * student_gain[l]
            through = scale * scaled - wide * scale**3 * jnp.mean(
                wide * scaled, axis=-1, keepdims=True
            )
            grad_rows = grad_rows + through + c_rows[l - 1]
        down = contract_rows(units[l], by_owner(grad_out)).astype(BF16)
        half = ds // 2
        down = down[:, :half].astype(F32) + swap(down[:, half:]).astype(F32)
        down_grads[l] = reduce_blocks([down[:, i * slot : (i + 1) * slot] for i in range(chips)])
        acts = jnp.concatenate([grad_gate_act, grad_up_act], axis=1)
        both = contract_rows(by_owner(normeds[l]), acts).astype(BF16)
        both = both[:half].astype(F32) + swap(both[half:]).astype(F32)
        both = reduce_blocks([both[i * slot : (i + 1) * slot] for i in range(chips)])
        width = grad_gate_act.shape[1]
        gate_grads[l] = both[:, :width]
        up_grads[l] = both[:, width:]

    lefts, rights = [], []
    for l in range(s_layers):
        found = [deltas[l][:, :share]]
        for k in range(1, n):
            found.append(push(deltas[l][:, k * share : (k + 1) * share], "tensor", k))
        ordered = [found[(n - k) % n] for k in range(n)]
        rights += [b[:own] for b in ordered] + [b[own:] for b in ordered]
        pair = [states[l + 1], swap(states[l + 1])]
        lefts += [take_blocks(s, 1, 2 * slot, groups) for s in pair]
    wide = contract_rows(jnp.concatenate(lefts), jnp.concatenate(rights))
    wide = reduce_blocks([wide[i * 2 * slot : (i + 1) * 2 * slot] for i in range(chips)])
    kept = jnp.where(core == 0, wide[:slot], wide[slot:])
    given = jnp.where(core == 0, wide[slot:], wide[:slot])
    other = swap(given)
    grad_proj = jnp.concatenate(
        [jnp.where(core == 0, kept, other), jnp.where(core == 0, other, kept)], axis=1
    )

    grad_gate, grad_up, grad_down = jnp.stack(gate_grads), jnp.stack(up_grads), jnp.stack(down_grads)
    sums = jnp.stack(
        error_parts + [jnp.sum(g * g) for g in (grad_gate, grad_up, grad_down, grad_proj)]
    )
    sums = sums + swap(sums)
    got = sums
    for s in shifts[1:]:
        got = got + push_chip(sums, s)
    sums = got
    for k in range(1, n):
        got = got + push(sums, "tensor", k)
    groups_n = 2 * chips
    mean_error = got[:s_layers] / (tokens * groups_n * dt)
    entries = s_layers * ds * s_gate.shape[2] * n
    counts = jnp.array([entries, entries, entries, ds * dt], F32)
    grad_rms = jnp.sqrt(got[s_layers:] / counts)
    return (jnp.stack(out_states), grad_gate, grad_up, grad_down, grad_proj, mean_error, grad_rms)


def solution(mesh):
    dp, n = mesh.shape["dp"], mesh.shape["tensor"]
    view = Mesh(mesh.devices.reshape(dp // 4, 2, 2, n), ("row", "col", "core", "tensor"))
    every = ("row", "col", "core")
    return jax.shard_map(
        per_device,
        mesh=view,
        in_specs=(
            P(every, None),
            P(),
            P(None, every, "tensor"),
            P(None, every, "tensor"),
            P(None, "tensor", every),
            P(every, None),
            P(),
            P(None, None, "tensor"),
            P(None, None, "tensor"),
            P(None, "tensor", None),
            P(None, "tensor"),
            P(),
        ),
        out_specs=(
            P(None, (*every, "tensor"), None),
            P(None, every, "tensor"),
            P(None, every, "tensor"),
            P(None, "tensor", every),
            P(every, "tensor"),
            P(),
            P(),
        ),
        check_vma=False,
    )
```

```python
import jax
import jax.numpy as jnp
from jax import lax
from jax.sharding import Mesh
from jax.sharding import PartitionSpec as P

SEQ = 512
EPSILON = 1e-05
F32 = jnp.float32
BF16 = jnp.bfloat16
CHIP = ("row", "col")


def inverse_rms(values):
    return lax.rsqrt(jnp.mean(values * values, axis=-1, keepdims=True) + EPSILON)


def dot(left, right):
    return jnp.dot(left, right, preferred_element_type=F32)


def contract_rows(left, right):
    return lax.dot_general(left, right, (((0,), (0,)), ((), ())), preferred_element_type=F32)


def contract_cols(left, right):
    return lax.dot_general(left, right, (((1,), (1,)), ((), ())), preferred_element_type=F32)


def pull(value, axis, shift):
    n = lax.axis_size(axis)
    return lax.ppermute(value, axis, [(j, (j - shift) % n) for j in range(n)])


def push(value, axis, shift):
    n = lax.axis_size(axis)
    return lax.ppermute(value, axis, [(j, (j + shift) % n) for j in range(n)])


def swap(value):
    return lax.ppermute(value, "core", [(0, 1), (1, 0)])


def chip_shifts():
    return [(r, c) for r in range(lax.axis_size("row")) for c in range(lax.axis_size("col"))]


def push_chip(value, shift):
    rows, cols = lax.axis_size("row"), lax.axis_size("col")
    pairs = [
        (r * cols + c, ((r + shift[0]) % rows) * cols + (c + shift[1]) % cols)
        for r in range(rows)
        for c in range(cols)
    ]
    return lax.ppermute(value, CHIP, pairs)


def chip_index(shift):
    rows, cols = lax.axis_size("row"), lax.axis_size("col")
    row = lax.rem(lax.axis_index("row") + shift[0], rows)
    col = lax.rem(lax.axis_index("col") + shift[1], cols)
    return row * cols + col


def after(value, *others):
    return lax.optimization_barrier((value, *others))[0]


def pull_lines(block):
    rows, cols = lax.axis_size("row"), lax.axis_size("col")
    found = {(0, 0): block}
    for c in range(1, cols):
        found[(0, c)] = pull(block, "col", c)
    for r in range(1, rows):
        found[(r, 0)] = pull(block, "row", r)
    return found


def pull_rest(found, axis):
    rows, cols = lax.axis_size("row"), lax.axis_size("col")
    half = found[(0, 0)].shape[axis] // 2
    for r in range(1, rows):
        for c in range(1, cols):
            first = lax.slice_in_dim(found[(0, c)], 0, half, axis=axis)
            last = lax.slice_in_dim(found[(r, 0)], half, None, axis=axis)
            found[(r, c)] = jnp.concatenate(
                [pull(first, "row", r), pull(last, "col", c)], axis=axis
            )
    return [found[s] for s in chip_shifts()]


def take_blocks(value, axis, width, starts):
    return jnp.concatenate(
        [lax.dynamic_slice_in_dim(value, s * width, width, axis) for s in starts], axis=axis
    )


def per_device(
    teacher_in,
    teacher_gain,
    t_gate,
    t_up,
    t_down,
    student_in,
    student_gain,
    s_gate,
    s_up,
    s_down,
    proj,
    layer_map,
):
    n = lax.axis_size("tensor")
    pos = lax.axis_index("tensor")
    core = lax.axis_index("core")
    shifts = chip_shifts()
    chips = len(shifts)
    t_layers = t_gate.shape[0]
    s_layers = s_gate.shape[0]
    tokens, dt = teacher_in.shape
    ds = student_in.shape[1]
    own = tokens // n
    share = dt // (2 * chips)
    positions = [lax.rem(pos + k, n) for k in range(n)]
    groups = [chip_index(s) for s in shifts]
    mine_cols = [g * 2 + core for g in groups]
    other_cols = [g * 2 + 1 - core for g in groups]

    def sum_rows(part):
        total = part[:own].astype(F32)
        for k in range(1, n):
            total = total + push(part[k * own : (k + 1) * own], "tensor", k).astype(F32)
        return total

    def gather_rows(rows):
        return jnp.concatenate([rows] + [pull(rows, "tensor", k) for k in range(1, n)])

    pairs = [jnp.concatenate([t_gate[k], t_up[k]], axis=1) for k in range(t_layers)]
    weights, gate = [], ()
    for k in range(t_layers):
        near = pull_lines(after(pairs[k], *gate) if gate else pairs[k])
        near_down = pull_lines(after(t_down[k], *gate[:1]) if gate else t_down[k])
        full = pull_rest(near, 0)
        full_down = pull_rest(near_down, 1)
        weights.append((full, full_down))
        gate = (full[-1],)

    proj_mine = lax.dynamic_slice_in_dim(proj, core * share, share, 1)
    proj_blocks = {k: pull(proj_mine, "tensor", k) for k in range(1, n) if k in (1, n - 1)}

    x = take_blocks(student_in, 0, own, positions)
    states, x_rows = [x], [x[:own].astype(F32)]
    normeds, gate_slopes, up_slopes, units, scales = [], [], [], [], []
    for l in range(s_layers):
        wide = states[l].astype(F32)
        scale = inverse_rms(wide)
        normed = (wide * scale * student_gain[l]).astype(BF16)
        gate_act = dot(normed, s_gate[l])
        up_act = dot(normed, s_up[l])
        sigma = jax.nn.sigmoid(gate_act)
        silu = gate_act * sigma
        unit = (silu * up_act).astype(BF16)
        part = dot(unit, s_down[l]).astype(BF16)
        next_rows = (x_rows[l] + sum_rows(part)).astype(BF16)
        x_rows.append(next_rows.astype(F32))
        states.append(gather_rows(next_rows))
        normeds.append(normed)
        gate_slopes.append(up_act * sigma * (1.0 + gate_act * (1.0 - sigma)))
        up_slopes.append(silu)
        units.append(unit)
        scales.append(scale[:own])

    wide = teacher_in.astype(F32)
    normed = (wide * inverse_rms(wide) * teacher_gain[0]).astype(BF16)
    normed = take_blocks(normed, 0, own, positions)
    kept = take_blocks(normed, 1, share, mine_cols)
    given = take_blocks(normed, 1, share, other_cols)
    normed = jnp.concatenate([kept, swap(given)])
    rows = lax.dynamic_slice_in_dim(teacher_in, pos * own, own, 0)
    state = jnp.concatenate(
        [take_blocks(rows, 1, share, mine_cols), swap(take_blocks(rows, 1, share, other_cols))]
    ).astype(F32)
    gain_mine = take_blocks(teacher_gain, 1, share, mine_cols)
    home = [lax.axis_index("row"), lax.axis_index("col")]

    def to_plain(value, first):
        rows_n, cols_n = lax.axis_size("row"), lax.axis_size("col")
        picked = []
        for k in range(chips):
            chip = lax.rem(first + k, chips)
            r = lax.rem(chip // cols_n - home[0] + rows_n, rows_n)
            c = lax.rem(lax.rem(chip, cols_n) - home[1] + cols_n, cols_n)
            picked.append(r * cols_n + c)
        return take_blocks(value, 1, share, picked)

    narrows = []
    for k in range(t_layers):
        w_pair, w_down = weights[k]
        total = dot(normed[:, :share], w_pair[0])
        for i in range(1, chips):
            total = total + dot(normed[:, i * share : (i + 1) * share], w_pair[i])
        acts = total[:tokens] + swap(total[tokens:])
        width = t_gate.shape[2]
        hidden = (jax.nn.silu(acts[:, :width]) * acts[:, width:]).astype(BF16)
        both = jnp.concatenate([hidden, swap(hidden)])
        part = jnp.concatenate([dot(both, w).astype(BF16) for w in w_down], axis=1)

        def rows_of(j):
            return jnp.concatenate(
                [part[j * own : (j + 1) * own], part[tokens + j * own : tokens + (j + 1) * own]]
            )

        total = rows_of(0).astype(F32)
        for j in range(1, n):
            total = total + push(rows_of(j), "tensor", j).astype(F32)
        narrow = (state + total).astype(BF16)
        narrows.append(narrow)
        state = narrow.astype(F32)
        if k + 1 < t_layers:
            squares = jnp.sum(state * state, axis=-1, keepdims=True)
            across = swap(jnp.concatenate([squares[own:], squares[:own]]))
            inv = lax.rsqrt((squares + across) / dt + EPSILON)
            block = (state * inv * gain_mine[k + 1]).astype(BF16)
            blocks = [block] + [pull(block, "tensor", j) for j in range(1, n)]
            normed = jnp.concatenate([b[:own] for b in blocks] + [b[own:] for b in blocks])
            if len(proj_blocks) < n - 1:
                for j in range(2, n - 1):
                    proj_blocks[j] = pull(after(proj_mine, normed), "tensor", j)

    proj_cols = jnp.concatenate([proj_mine] + [proj_blocks[k] for k in range(1, n)], axis=1)
    row_pairs = []
    for l in range(s_layers):
        rows = x_rows[l + 1].astype(BF16)
        row_pairs.append(jnp.concatenate([rows, swap(rows)]))
    student_of = jnp.sum(
        jnp.where(
            layer_map[None, :] == jnp.arange(t_layers)[:, None], jnp.arange(s_layers)[None, :], 0
        ),
        axis=1,
    )
    row_pairs = jnp.stack(row_pairs)
    predicted = [
        dot(lax.dynamic_index_in_dim(row_pairs, student_of[k], 0, keepdims=False), proj_cols)
        for k in range(t_layers)
    ]
    error_parts, deltas, c_rows = [], [], []
    for k in range(t_layers):
        errors = predicted[k] - to_plain(narrows[k], pos).astype(F32)
        error_parts.append(jnp.sum(errors * errors))
        deltas.append((errors * (2.0 / (s_layers * SEQ))).astype(BF16))
        part = contract_cols(deltas[k], proj_cols)
        c_rows.append(part[:own] + swap(part[own:]))
    c_rows = jnp.stack(c_rows)
    c_rows = [
        lax.dynamic_index_in_dim(c_rows, layer_map[l], 0, keepdims=False) for l in range(s_layers)
    ]

    ds_mine = [g * 2 + core for g in groups]
    ds_other = [g * 2 + 1 - core for g in groups]
    slot = ds // (2 * chips)
    half = ds // 2

    def by_owner(value):
        return take_blocks(value, 1, slot, ds_mine + ds_other)

    rows_n, cols_n = lax.axis_size("row"), lax.axis_size("col")

    def first_sums(blocks, axis):
        mid = blocks[0].shape[axis] // 2
        grid = [blocks[r * cols_n : (r + 1) * cols_n] for r in range(rows_n)]
        left = [[lax.slice_in_dim(b, 0, mid, axis=axis) for b in line] for line in grid]
        right = [[lax.slice_in_dim(b, mid, None, axis=axis) for b in line] for line in grid]
        lines = jnp.concatenate([line[0] for line in left])
        for c in range(1, cols_n):
            sent = jnp.concatenate([line[c] for line in left]).astype(BF16)
            lines = lines + push(sent, "col", c).astype(F32)
        columns = jnp.concatenate(right[0])
        for r in range(1, rows_n):
            sent = jnp.concatenate(right[r]).astype(BF16)
            columns = columns + push(sent, "row", r).astype(F32)
        return lines, columns

    def last_sums(lines, columns, axis):
        size = lines.shape[0] // rows_n
        left = lines[:size]
        for r in range(1, rows_n):
            sent = lines[r * size : (r + 1) * size].astype(BF16)
            left = left + push(sent, "row", r).astype(F32)
        right = columns[:size]
        for c in range(1, cols_n):
            sent = columns[c * size : (c + 1) * size].astype(BF16)
            right = right + push(sent, "col", c).astype(F32)
        return jnp.concatenate([left, right], axis=axis)

    gate_grads = [None] * s_layers
    up_grads = [None] * s_layers
    down_grads = [None] * s_layers
    grad_rows = c_rows[s_layers - 1]
    owned = [by_owner(v) for v in normeds]
    waiting = []
    for l in reversed(range(s_layers)):
        narrow_rows = grad_rows.astype(BF16)
        waiting = [(f, after(x, narrow_rows), after(y, narrow_rows)) for f, x, y in waiting]
        grad_out = gather_rows(narrow_rows)
        grad_units = contract_cols(grad_out, s_down[l])
        grad_gate_act = (grad_units * gate_slopes[l]).astype(BF16)
        grad_up_act = (grad_units * up_slopes[l]).astype(BF16)
        later = grad_out
        if l > 0:
            norm_part = contract_cols(grad_gate_act, s_gate[l]) + contract_cols(
                grad_up_act, s_up[l]
            )
            norm_part = norm_part.astype(BF16)
            later = after(grad_out, norm_part)
            grad_norm = sum_rows(norm_part)
            wide = x_rows[l]
            scale = scales[l]
            scaled = grad_norm * student_gain[l]
            through = scale * scaled - wide * scale**3 * jnp.mean(
                wide * scaled, axis=-1, keepdims=True
            )
            grad_rows = grad_rows + through + c_rows[l - 1]
        down = contract_rows(units[l], by_owner(later)).astype(BF16)
        down = down[:, :half].astype(F32) + swap(down[:, half:]).astype(F32)
        lines, columns = first_sums([down[:, i * slot : (i + 1) * slot] for i in range(chips)], 0)

        def keep_down(lines, columns, l=l):
            down_grads[l] = last_sums(lines, columns, 0)

        waiting.append((keep_down, lines, columns))
        acts = jnp.concatenate([grad_gate_act, grad_up_act], axis=1)
        if l > 0:
            acts = after(acts, norm_part)
        both = contract_rows(owned[l], acts).astype(BF16)
        both = both[:half].astype(F32) + swap(both[half:]).astype(F32)
        lines, columns = first_sums([both[i * slot : (i + 1) * slot] for i in range(chips)], 1)

        def keep_pair(lines, columns, l=l):
            both = last_sums(lines, columns, 1)
            gate_grads[l] = both[:, : both.shape[1] // 2]
            up_grads[l] = both[:, both.shape[1] // 2 :]

        waiting.append((keep_pair, lines, columns))
        if l == s_layers - 1:
            gathered = grad_out
    for f, lines, columns in waiting:
        f(lines, columns)

    lefts, rights = [], []
    full_states = []
    for l in range(s_layers):
        full_states.append(
            jnp.concatenate(
                [take_blocks(s, 1, 2 * slot, groups) for s in (states[l + 1], swap(states[l + 1]))]
            )
        )
    full_states = jnp.stack(full_states)
    wide = None
    for k in range(t_layers):
        delta = deltas[k] if k + 1 < t_layers else after(deltas[k], gathered)
        found = [delta[:, :share]]
        for j in range(1, n):
            found.append(push(delta[:, j * share : (j + 1) * share], "tensor", j))
        ordered = [found[(n - j) % n] for j in range(n)]
        right = jnp.concatenate([b[:own] for b in ordered] + [b[own:] for b in ordered])
        left = lax.dynamic_index_in_dim(full_states, student_of[k], 0, keepdims=False)
        term = contract_rows(left, right)
        wide = term if wide is None else wide + term
    lines, columns = first_sums([wide[i * 2 * slot : (i + 1) * 2 * slot] for i in range(chips)], 1)
    wide = last_sums(lines, columns, 1)
    kept = jnp.where(core == 0, wide[:slot], wide[slot:])
    given = jnp.where(core == 0, wide[slot:], wide[:slot])
    other = swap(given)
    grad_proj = jnp.concatenate(
        [jnp.where(core == 0, kept, other), jnp.where(core == 0, other, kept)], axis=1
    )

    out_states = []
    for k in range(t_layers):
        narrow = narrows[k] if k + 1 < t_layers else after(narrows[k], gathered)
        mine = to_plain(narrow[:own], 0)
        theirs = swap(to_plain(narrow[own:], 0))
        lower = jnp.where(core == 0, mine, theirs)
        upper = jnp.where(core == 0, theirs, mine)
        pieces = []
        for j in range(chips):
            pieces.append(lower[:, j * share : (j + 1) * share])
            pieces.append(upper[:, j * share : (j + 1) * share])
        out_states.append(jnp.concatenate(pieces, axis=1))

    lane = lax.broadcasted_iota(jnp.int32, (1, 128), 1)
    sums = jnp.zeros((1, 128), F32)
    for k in range(t_layers):
        sums = sums + jnp.where(lane == student_of[k], error_parts[k], 0.0)
    for i, grads in enumerate((gate_grads, up_grads, down_grads, [grad_proj])):
        for g in grads:
            sums = sums + jnp.where(lane == s_layers + i, jnp.sum(g * g), 0.0)
    sums = sums + swap(sums)
    got = sums
    for s in shifts[1:]:
        got = got + push_chip(sums, s)
    sums = got
    for k in range(1, n):
        got = got + push(sums, "tensor", k)
    mean_error = got[0, :s_layers] / (tokens * 2 * chips * dt)
    entries = s_layers * ds * s_gate.shape[2] * n
    counts = jnp.array([entries, entries, entries, ds * dt], F32)
    grad_rms = jnp.sqrt(got[0, s_layers : s_layers + 4] / counts)
    return (
        jnp.stack(out_states),
        jnp.stack(gate_grads),
        jnp.stack(up_grads),
        jnp.stack(down_grads),
        grad_proj,
        mean_error,
        grad_rms,
    )


def solution(mesh):
    dp, n = mesh.shape["dp"], mesh.shape["tensor"]
    view = Mesh(mesh.devices.reshape(dp // 4, 2, 2, n), ("row", "col", "core", "tensor"))
    every = ("row", "col", "core")
    return jax.shard_map(
        per_device,
        mesh=view,
        in_specs=(
            P(every, None),
            P(),
            P(None, every, "tensor"),
            P(None, every, "tensor"),
            P(None, "tensor", every),
            P(every, None),
            P(),
            P(None, None, "tensor"),
            P(None, None, "tensor"),
            P(None, "tensor", None),
            P(None, "tensor"),
            P(),
        ),
        out_specs=(
            P(None, (*every, "tensor"), None),
            P(None, every, "tensor"),
            P(None, every, "tensor"),
            P(None, "tensor", every),
            P(every, "tensor"),
            P(),
            P(),
        ),
        check_vma=False,
    )
```
